256 devices in a mesh: narrow: 8 (over x, core), wide: 32 (over y, z).
Axes of the slice: x: 4, y: 4, z: 8, core: 2. Of those that a mesh axis runs over, the one named last changes fastest.
Arguments:
- block_ids: int32 [4096, 4], P(('narrow', 'wide')), may hold values from 0 to 511, as said below
- incidence: int32 [4096, 4, 128, 128], P(('narrow', 'wide')), may hold values from 0 to 1
- costs: int32 [4096, 128], P(('narrow', 'wide')), may hold values from 16 to 80
- start_mult: float32 [512, 128], replicated, may hold values from 0.25 to 4
- upper: float32 [1], replicated, may hold values from 65536 to 131072
Outputs:
- multipliers: float32 [512, 128], replicated
- primal_mean: float32 [4096, 128], P(('narrow', 'wide'))
The draws below stay inside these ranges and needn't reach their ends.
Inputs may be any that keep to these rules, and one draw needn't show every extreme that they name: `block_ids`: the 4 row blocks listed for one tile are distinct.
All inputs are finite; a program needn't handle non-finite values.
Results may differ from the reference program's by a relative error of at most 0.0003.
Values sent between devices are 32-bit elements; how exact they have to be, the bound alone decides.
No kernel may reach another device: no remote copies, remote signals or barrier semaphores. Data moves between devices by JAX's collectives and lax.ppermute only.
A program may use at most 64 MiB of HBM per device.

```python
import math
import jax
import jax.numpy as jnp
from jax import lax

BLK = 128
TILE = 128
K = 4
TILES_DEV = 16
ITERS = 3
RB = 512
TILES = 4096


def pick_blocks(key):
    random_part = jax.random.randint(jax.random.fold_in(key, 17), (TILES, RB), 0, 4096)
    ranking = random_part * RB + jnp.arange(RB, dtype=jnp.int32)[None, :]
    _, chosen = lax.top_k(ranking, K)
    return chosen.astype(jnp.int32)


def draw_block_ids(key, part):
    return pick_blocks(key)


def draw_incidence(key, part):
    chosen = pick_blocks(key)
    levels = jax.random.randint(jax.random.fold_in(key, 29), (RB, BLK), 1, 9)
    row_level = jnp.take(levels, chosen, axis=0)
    entries = jax.random.randint(jax.random.fold_in(key, 31), (TILES, K, BLK, TILE), 0, K * BLK // 2)
    return (entries < row_level[:, :, :, None]).astype(jnp.int32)


def touch_ends(values, rng, low, top_value):
    spot = [jax.random.randint(jax.random.fold_in(rng, axis), (), 0, length) for axis, length in enumerate(values.shape)]
    longest = values.shape.index(max(values.shape))
    beside = spot[:longest] + [(spot[longest] + 1) % values.shape[longest]] + spot[longest + 1:]
    return values.at[tuple(spot)].set(low).at[tuple(beside)].set(top_value)


def setup_inputs(seed: int = 0) -> dict:
    key_list = jax.random.split(jax.random.key(seed), 6)
    return {
        "block_ids": draw_block_ids(jax.random.fold_in(key_list[5], 71), 0),
        "incidence": draw_incidence(jax.random.fold_in(key_list[5], 71), 0),
        "costs": touch_ends(jax.random.randint(key_list[2], (TILES, TILE), 16, 81), jax.random.fold_in(key_list[2], 1), 16, 80).astype(jnp.int32),
        "start_mult": jnp.clip(jnp.exp(jax.random.uniform(key_list[3], (RB, BLK), jnp.float32, math.log(0.25), math.log(4.0))), 0.25, 4.0),
        "upper": jnp.clip(jax.random.uniform(key_list[4], (1,), jnp.float32, 65536.0, 131072.0), 65536.0, 131072.0),
    }


def reference(block_ids, incidence, costs, start_mult, upper):
    groups = TILES // TILES_DEV
    ids_g = block_ids.reshape(groups, TILES_DEV, K)
    inc_g = incidence.reshape(groups, TILES_DEV, K, BLK, TILE)
    cost_g = costs.reshape(groups, TILES_DEV, TILE).astype(jnp.float32)
    mult = start_mult
    primal_mean = jnp.zeros((groups, TILES_DEV, TILE), jnp.float32)
    hi = lax.Precision.HIGHEST
    for step in range(ITERS):
        def reduce_cols(args):
            ids, inc, cost = args
            u_tile = jnp.take(mult, ids, axis=0)
            incf = inc.astype(jnp.float32)
            return cost - jnp.einsum('tkrc,tkr->tc', incf, u_tile, precision=hi)

        reduced = lax.map(reduce_cols, (ids_g, inc_g, cost_g))
        primal = 1.0 / (1.0 + jnp.exp(reduced / 8.0))
        soft = jnp.sum(-8.0 * jax.nn.softplus(-reduced / 8.0))
        value = jnp.sum(mult) + soft
        if step == 0:
            primal_mean = primal
        else:
            primal_mean = 0.3 * primal + 0.7 * primal_mean

        def add_cover(total, args):
            ids, inc, pm = args
            incf = inc.astype(jnp.float32)
            part = jnp.einsum('tkrc,tc->tkr', incf, pm, precision=hi).reshape(TILES_DEV * K, BLK)
            onehot = (ids.reshape(TILES_DEV * K, 1) == jnp.arange(RB, dtype=jnp.int32)[None, :]).astype(jnp.float32)
            return total + jnp.dot(onehot.T, part, precision=hi, preferred_element_type=jnp.float32), None

        cover, _ = lax.scan(add_cover, jnp.zeros((RB, BLK), jnp.float32), (ids_g, inc_g, primal_mean))
        slope = 1.0 - cover
        norm = jnp.sum(slope * slope)
        size = (upper[0] - value) / (norm + 1e-6)
        mult = jnp.maximum(0.0, mult + size * slope)
    return mult, primal_mean.reshape(TILES, TILE)
```

```python
import jax
import jax.numpy as jnp
from jax import lax
from jax.experimental import pallas as pl
from jax.experimental.pallas import tpu as pltpu
from jax.sharding import Mesh
from jax.sharding import PartitionSpec as P

BLK = 128
TILE = 128
K = 4
ITERS = 3
CHUNKS = 8
X, C, Y, Z = 4, 2, 4, 8
SPLIT = ("x", "c", "y", "z")
OWNERS = ("c", "x", "y")
NEAR = ("x", "y")
SLOT = 24

f32, bf16 = jnp.float32, jnp.bfloat16
VMEM = pl.BlockSpec(memory_space=pltpu.VMEM)
SMEM = pl.BlockSpec(memory_space=pltpu.SMEM)
HBM = pl.BlockSpec(memory_space=pltpu.HBM)


def three_parts(v):
    high = v.astype(bf16)
    rest = v - high.astype(f32)
    middle = rest.astype(bf16)
    return high, middle, (rest - middle.astype(f32)).astype(bf16)


def column_step(mult_ref, ids_ref, cost_ref, inc_tile, prev, rows_scr, parts_scr, mean_ref, soft_ref, cover_ref):
    tiles = cost_ref.shape[0]
    for k in range(K):
        for t in range(tiles):
            at = k * tiles + t
            rows_scr[at : at + 1, :] = mult_ref[pl.ds(ids_ref[t, k], 1), :]
    parts = three_parts(rows_scr[...])
    line = lax.broadcasted_iota(jnp.int32, (tiles, BLK), 0)
    acc = jnp.zeros((3 * tiles, TILE), f32)
    for t in range(tiles):
        keep = jnp.where(line == t, 1.0, 0.0).astype(bf16)
        lhs = jnp.concatenate(
            [
                jnp.concatenate([p[k * tiles : (k + 1) * tiles] * keep for k in range(K)], axis=1)
                for p in parts
            ],
            axis=0,
        )
        acc += jnp.dot(lhs, inc_tile(t), preferred_element_type=f32)
    priced = acc[:tiles] + acc[tiles : 2 * tiles] + acc[2 * tiles :]
    reduced = cost_ref[...].astype(f32) - priced
    scaled = reduced / 8.0
    primal = 1.0 / (1.0 + jnp.exp(scaled))
    soft = -8.0 * (jnp.maximum(-scaled, 0.0) + jnp.log1p(jnp.exp(-jnp.abs(scaled))))
    soft_ref[...] = soft[:8] + soft[8:]
    mean = primal if prev is None else 0.3 * primal + 0.7 * prev[...]
    mean_ref[...] = mean
    parts_scr[...] = jnp.zeros_like(parts_scr)
    for s, p in enumerate(three_parts(mean)):
        parts_scr[pl.ds(s, tiles, stride=8), :] = p.astype(f32)
    cover_ref[...] = jnp.zeros_like(cover_ref)
    for t in range(tiles):
        lhs = parts_scr[8 * t : 8 * (t + 1), :].astype(bf16)
        out = lax.dot_general(lhs, inc_tile(t), (((1,), (1,)), ((), ())), preferred_element_type=f32)
        part = out[0:1] + out[1:2] + out[2:3]
        for k in range(K):
            row = pl.ds(ids_ref[t, k], 1)
            cover_ref[row, :] += part[:, k * BLK : (k + 1) * BLK]


def first_kernel(ids_ref, inc_hbm, cost_ref, mult_ref, inc_ref, mean_ref, soft_ref, cover_ref, raw, rows_scr, parts_scr, sems):
    tiles = cost_ref.shape[0]
    each = tiles // CHUNKS
    copies = [
        pltpu.make_async_copy(inc_hbm.at[pl.ds(i * each, each)], raw.at[pl.ds(i * each, each)], sems.at[i])
        for i in range(CHUNKS)
    ]
    for copy in copies:
        copy.start()
    done = set()

    def inc_tile(t):
        if t not in done:
            done.add(t)
            if t % each == 0:
                copies[t // each].wait()
            inc_ref[t] = raw[t].reshape(K * BLK, TILE).astype(f32).astype(bf16)
        return inc_ref[t]

    column_step(mult_ref, ids_ref, cost_ref, inc_tile, None, rows_scr, parts_scr, mean_ref, soft_ref, cover_ref)


def row_step(own_ref, other_ref, mult_ref, upper_ref, new_ref):
    me = lax.axis_index("c")
    n, half = own_ref.shape[0], mult_ref.shape[0] // 2
    slopes, soft, norm = [], 0.0, 0.0
    for ref in (own_ref, other_ref):
        slope = 1.0 - ref[:, : SLOT - 8, :].reshape(half, BLK)
        slopes.append(slope)
        norm = norm + jnp.sum((slope * slope).reshape(half // 8, 8, BLK), axis=0)
        soft = soft + jnp.sum(ref[:, SLOT - 8 :, :], axis=0)
    total = jnp.sum(mult_ref[...].reshape(half // 4, 8, BLK), axis=0) + soft
    value = jnp.sum(total, keepdims=True)
    size = (upper_ref[0] - value) / (jnp.sum(norm, keepdims=True) + 1e-06)
    for slope, core in zip(slopes, (me, 1 - me)):
        at = pl.ds(pl.multiple_of(core * half, half), half)
        new_ref[at, :] = jnp.maximum(0.0, mult_ref[at, :] + size * slope)


def next_kernel(own_ref, other_ref, mult_ref, upper_ref, ids_ref, inc_ref, cost_ref, prev_ref, new_ref, mean_ref, soft_ref, cover_ref, rows_scr, parts_scr):
    row_step(own_ref, other_ref, mult_ref, upper_ref, new_ref)
    column_step(new_ref, ids_ref, cost_ref, lambda t: inc_ref[t], prev_ref, rows_scr, parts_scr, mean_ref, soft_ref, cover_ref)


def owner_kernel(in_ref, soft_ref, out_ref):
    total = in_ref[0]
    for i in range(1, in_ref.shape[0]):
        total += in_ref[i]
    for i in range(out_ref.shape[0]):
        out_ref[i, : SLOT - 8] = total
        out_ref[i, SLOT - 8 :] = soft_ref[...]


def spread_kernel(in_ref, out_ref):
    total = in_ref[0]
    for i in range(1, in_ref.shape[0]):
        total += in_ref[i]
    for i in range(out_ref.shape[0]):
        out_ref[i] = total


def call(kernel, name, out, specs, scratch=(), mib=8):
    return pl.pallas_call(
        kernel,
        out_shape=out,
        in_specs=specs,
        out_specs=jax.tree.map(lambda _: VMEM, out),
        scratch_shapes=scratch,
        compiler_params=pltpu.CompilerParams(vmem_limit_bytes=mib << 20),
        name=name,
    )


def local(block_ids, incidence, costs, start_mult, upper):
    tiles, rows = block_ids.shape[0], start_mult.shape[0]
    sds = jax.ShapeDtypeStruct
    columns = (sds((tiles, TILE), f32), sds((8, TILE), f32), sds((rows, BLK), f32))
    scratch = [pltpu.VMEM((tiles * K, BLK), f32), pltpu.VMEM((tiles * 8, TILE), f32)]
    inc, mean, soft, cover = call(
        first_kernel,
        "first",
        (sds((tiles, K * BLK, TILE), bf16), *columns),
        [SMEM, HBM, VMEM, VMEM],
        [pltpu.VMEM((tiles, K, BLK, TILE), jnp.int32), *scratch, pltpu.SemaphoreType.DMA((CHUNKS,))],
        mib=16,
    )(block_ids, incidence, costs, start_mult)
    mult = start_mult
    for step in range(ITERS):
        there = lax.all_to_all(cover.reshape(C * X * Y, SLOT - 8, BLK), OWNERS, 0, 0, tiled=True)
        there = call(owner_kernel, "owner", sds((Z, SLOT, BLK), f32), [VMEM] * 2)(there, soft)
        there = lax.all_to_all(there, "z", 0, 0, tiled=True)
        there = call(spread_kernel, "spread", sds((X * Y, SLOT, BLK), f32), [VMEM])(there)
        own = lax.all_to_all(there, NEAR, 0, 0, tiled=True)
        other = lax.ppermute(own, "c", [(0, 1), (1, 0)])
        if step < ITERS - 1:
            mult, mean, soft, cover = call(
                next_kernel,
                "next",
                (sds((rows, BLK), f32), *columns),
                [VMEM] * 3 + [SMEM] * 2 + [VMEM] * 3,
                scratch,
            )(own, other, mult, upper, block_ids, inc, costs, mean)
    mult = call(row_step, "last", sds((rows, BLK), f32), [VMEM] * 3 + [SMEM])(own, other, mult, upper)
    return mult, mean


def solution(mesh):
    split = Mesh(mesh.devices.reshape(X, C, Y, Z), SPLIT)
    return jax.shard_map(
        local,
        mesh=split,
        in_specs=(
            P(SPLIT, None),
            P(SPLIT, None, None, None),
            P(SPLIT, None),
            P(),
            P(),
        ),
        out_specs=(P(), P(SPLIT, None)),
        check_vma=False,
    )
```

```python
import jax
import jax.numpy as jnp
from jax import lax
from jax.experimental import pallas as pl
from jax.experimental.pallas import tpu as pltpu
from jax.sharding import Mesh
from jax.sharding import PartitionSpec as P

BLK = 128
TILE = 128
K = 4
ITERS = 3
CHUNKS = 8
X, C, Y, Z = 4, 2, 4, 8
SPLIT = ("x", "c", "y", "z")
OWNERS = ("c", "x", "y")
NEAR = ("x", "y")
SLOT = 24

f32, bf16 = jnp.float32, jnp.bfloat16
VMEM = pl.BlockSpec(memory_space=pltpu.VMEM)
SMEM = pl.BlockSpec(memory_space=pltpu.SMEM)
HBM = pl.BlockSpec(memory_space=pltpu.HBM)


def three_parts(v):
    high = v.astype(bf16).astype(f32)
    rest = v - high
    middle = rest.astype(bf16).astype(f32)
    return high, middle, rest - middle


def column_step(mult_ref, ids_ref, cost_ref, inc_tile, prev, rows_scr, parts_scr, mean_ref, soft_ref, cover_ref):
    tiles = cost_ref.shape[0]
    for t in range(tiles):
        for k in range(K):
            at = (t // 8 * K + k) * 8 + t % 8
            rows_scr[at : at + 1, :] = mult_ref[pl.ds(ids_ref[k, t], 1), :]
    parts_scr[...] = jnp.zeros_like(parts_scr)
    cover_ref[...] = jnp.zeros_like(cover_ref)
    line = lax.broadcasted_iota(jnp.int32, (8, BLK), 0)
    none = jnp.zeros((8, BLK), f32)
    soft_sum = none
    for group in range(tiles // 8):
        first = group * 8
        parts = [
            three_parts(rows_scr[(group * K + k) * 8 : (group * K + k + 1) * 8, :]) for k in range(K)
        ]
        acc = jnp.zeros((32, TILE), f32)
        for t in range(8):
            lhs = [
                jnp.concatenate([jnp.where(line == t, p, 0.0) for p in parts[k]] + [none], axis=0)
                for k in range(K)
            ]
            lhs = jnp.concatenate(lhs, axis=1).astype(bf16)
            acc += jnp.dot(lhs, inc_tile(first + t), preferred_element_type=f32)
        here = slice(first, first + 8)
        reduced = cost_ref[here, :].astype(f32) - (acc[:8] + acc[8:16] + acc[16:24])
        scaled = reduced / 8.0
        primal = 1.0 / (1.0 + jnp.exp(scaled))
        soft_sum += -8.0 * (jnp.maximum(-scaled, 0.0) + jnp.log1p(jnp.exp(-jnp.abs(scaled))))
        mean = primal if prev is None else 0.3 * primal + 0.7 * prev[here, :]
        mean_ref[here, :] = mean
        for s, p in enumerate(three_parts(mean)):
            parts_scr[pl.ds(first * 8 + s, 8, stride=8), :] = p
        for t in range(first, first + 8):
            lhs = parts_scr[8 * t : 8 * (t + 1), :].astype(bf16)
            out = lax.dot_general(
                lhs, inc_tile(t), (((1,), (1,)), ((), ())), preferred_element_type=f32
            )
            part = out[0:1] + out[1:2] + out[2:3]
            for k in range(K):
                cover_ref[pl.ds(ids_ref[k, t], 1), :] += part[:, k * BLK : (k + 1) * BLK]
    soft_ref[...] = soft_sum


def first_kernel(
    ids_hbm, inc_hbm, cost_hbm, mult_hbm, inc_ref, mean_ref, soft_ref, cover_ref,
    ids, raw, cost, mult, rows_scr, parts_scr, sems,
):
    tiles = cost.shape[0]
    each = tiles // CHUNKS
    small = [
        pltpu.make_async_copy(src, dst, sems.at[CHUNKS + i])
        for i, (src, dst) in enumerate(((ids_hbm, ids), (mult_hbm, mult), (cost_hbm, cost)))
    ]
    chunks = [
        pltpu.make_async_copy(
            inc_hbm.at[pl.ds(i * each, each)], raw.at[pl.ds(i * each, each)], sems.at[i]
        )
        for i in range(CHUNKS)
    ]
    for copy in small + chunks:
        copy.start()
    for copy in small:
        copy.wait()
    seen = set()

    def inc_tile(t):
        if t not in seen:
            seen.add(t)
            if t % each == 0:
                chunks[t // each].wait()
            inc_ref[t] = raw[t].reshape(K * BLK, TILE).astype(f32).astype(bf16)
        return inc_ref[t]

    column_step(mult, ids, cost, inc_tile, None, rows_scr, parts_scr, mean_ref, soft_ref, cover_ref)


def row_step(own_ref, other_ref, mult_ref, upper_ref, new_ref):
    me = lax.axis_index("c")
    n, half = own_ref.shape[0], mult_ref.shape[0] // 2
    slopes, soft, norm = [], 0.0, 0.0
    for ref in (own_ref, other_ref):
        slope = 1.0 - ref[:, : SLOT - 8, :].reshape(half, BLK)
        slopes.append(slope)
        norm = norm + jnp.sum((slope * slope).reshape(half // 8, 8, BLK), axis=0)
        soft = soft + jnp.sum(ref[:, SLOT - 8 :, :], axis=0)
    total = jnp.sum(mult_ref[...].reshape(half // 4, 8, BLK), axis=0) + soft
    value = jnp.sum(total, keepdims=True)
    size = (upper_ref[0] - value) / (jnp.sum(norm, keepdims=True) + 1e-06)
    for slope, core in zip(slopes, (me, 1 - me)):
        at = pl.ds(pl.multiple_of(core * half, half), half)
        new_ref[at, :] = jnp.maximum(0.0, mult_ref[at, :] + size * slope)


def next_kernel(own_ref, other_ref, mult_ref, upper_ref, ids_ref, inc_ref, cost_ref, prev_ref, new_ref, mean_ref, soft_ref, cover_ref, rows_scr, parts_scr):
    row_step(own_ref, other_ref, mult_ref, upper_ref, new_ref)
    column_step(new_ref, ids_ref, cost_ref, lambda t: inc_ref[t], prev_ref, rows_scr, parts_scr, mean_ref, soft_ref, cover_ref)


def owner_kernel(in_ref, soft_ref, out_ref):
    total = in_ref[0]
    for i in range(1, in_ref.shape[0]):
        total += in_ref[i]
    for i in range(out_ref.shape[0]):
        out_ref[i, : SLOT - 8] = total
        out_ref[i, SLOT - 8 :] = soft_ref[...]


def spread_kernel(in_ref, out_ref):
    total = in_ref[0]
    for i in range(1, in_ref.shape[0]):
        total += in_ref[i]
    for i in range(out_ref.shape[0]):
        out_ref[i] = total


def call(kernel, name, out, specs, scratch=(), mib=8):
    return pl.pallas_call(
        kernel,
        out_shape=out,
        in_specs=specs,
        out_specs=jax.tree.map(lambda _: VMEM, out),
        scratch_shapes=scratch,
        compiler_params=pltpu.CompilerParams(vmem_limit_bytes=mib << 20),
        name=name,
    )


def local(block_ids, incidence, costs, start_mult, upper):
    tiles, rows = block_ids.shape[0], start_mult.shape[0]
    sds = jax.ShapeDtypeStruct
    ids = block_ids.T
    columns = (sds((tiles, TILE), f32), sds((8, TILE), f32), sds((rows, BLK), f32))
    scratch = [pltpu.VMEM((tiles * K, BLK), f32), pltpu.VMEM((tiles * 8, TILE), f32)]
    inc, mean, soft, cover = call(
        first_kernel,
        "first",
        (sds((tiles, K * BLK, TILE), bf16), *columns),
        [HBM] * 4,
        [
            pltpu.SMEM((K, tiles), jnp.int32),
            pltpu.VMEM((tiles, K, BLK, TILE), jnp.int32),
            pltpu.VMEM((tiles, TILE), jnp.int32),
            pltpu.VMEM((rows, BLK), f32),
            *scratch,
            pltpu.SemaphoreType.DMA((CHUNKS + 3,)),
        ],
        mib=16,
    )(*(pltpu.with_memory_space_constraint(a, pltpu.HBM) for a in (ids, incidence, costs, start_mult)))
    mult = start_mult
    for step in range(ITERS):
        there = lax.all_to_all(cover.reshape(C * X * Y, SLOT - 8, BLK), OWNERS, 0, 0, tiled=True)
        there = call(owner_kernel, "owner", sds((Z, SLOT, BLK), f32), [VMEM] * 2)(there, soft)
        there = lax.all_to_all(there, "z", 0, 0, tiled=True)
        there = call(spread_kernel, "spread", sds((X * Y, SLOT, BLK), f32), [VMEM])(there)
        own = lax.all_to_all(there, NEAR, 0, 0, tiled=True)
        other = lax.ppermute(own, "c", [(0, 1), (1, 0)])
        if step < ITERS - 1:
            mult, mean, soft, cover = call(
                next_kernel,
                "next",
                (sds((rows, BLK), f32), *columns),
                [VMEM] * 3 + [SMEM] * 2 + [VMEM] * 3,
                scratch,
            )(own, other, mult, upper, ids, inc, costs, mean)
    mult = call(row_step, "last", sds((rows, BLK), f32), [VMEM] * 3 + [SMEM])(own, other, mult, upper)
    return mult, mean


def solution(mesh):
    split = Mesh(mesh.devices.reshape(X, C, Y, Z), SPLIT)
    return jax.shard_map(
        local,
        mesh=split,
        in_specs=(
            P(SPLIT, None),
            P(SPLIT, None, None, None),
            P(SPLIT, None),
            P(),
            P(),
        ),
        out_specs=(P(), P(SPLIT, None)),
        check_vma=False,
    )
```

```python
import jax
import jax.numpy as jnp
from jax import lax
from jax.experimental import pallas as pl
from jax.experimental.pallas import tpu as pltpu
from jax.sharding import Mesh
from jax.sharding import PartitionSpec as P

BLK = 128
TILE = 128
K = 4
ITERS = 3
X, C, Y, Z = 4, 2, 4, 8
SPLIT = ("x", "c", "y", "z")
OWNERS = ("c", "x", "y")
NEAR = ("x", "y")
SLOT = 24

f32, bf16 = jnp.float32, jnp.bfloat16
INC = bf16
VMEM = pl.BlockSpec(memory_space=pltpu.VMEM)
SMEM = pl.BlockSpec(memory_space=pltpu.SMEM)
HBM = pl.BlockSpec(memory_space=pltpu.HBM)


def three_parts(v):
    high = v.astype(bf16).astype(f32)
    rest = v - high
    middle = rest.astype(bf16).astype(f32)
    return high, middle, rest - middle


def column_step(mult_ref, ids_ref, cost_ref, inc_pair, prev, rows_scr, parts_scr, mean_ref, soft_ref, cover_ref):
    tiles = cost_ref.shape[0]
    for t in range(tiles):
        for k in range(K):
            at = (t // 8 * K + k) * 8 + t % 8
            rows_scr[at : at + 1, :] = mult_ref[pl.ds(ids_ref[k, t], 1), :]
    parts_scr[...] = jnp.zeros_like(parts_scr)
    cover_ref[...] = jnp.zeros_like(cover_ref)
    line = lax.broadcasted_iota(jnp.int32, (8, BLK), 0)
    none = jnp.zeros((8, BLK), f32)
    soft_sum = none
    for group in range(tiles // 8):
        parts = [
            three_parts(rows_scr[(group * K + k) * 8 : (group * K + k + 1) * 8, :]) for k in range(K)
        ]
        acc = jnp.zeros((32, 2 * TILE), f32)
        for q in range(4):
            keep = line % 4 == q
            lhs = [
                jnp.concatenate([jnp.where(keep, p, 0.0) for p in parts[k]] + [none], axis=0)
                for k in range(K)
            ]
            lhs = jnp.concatenate(lhs, axis=1).astype(bf16)
            acc += jnp.dot(lhs, inc_pair(group, q), preferred_element_type=f32)
        here = slice(group * 8, group * 8 + 8)
        both = acc[:8] + acc[8:16] + acc[16:24]
        priced = jnp.where(line < 4, both[:, :TILE], both[:, TILE:])
        reduced = cost_ref[here, :].astype(f32) - priced
        scaled = reduced / 8.0
        primal = 1.0 / (1.0 + jnp.exp(scaled))
        soft_sum += -8.0 * (jnp.maximum(-scaled, 0.0) + jnp.log1p(jnp.exp(-jnp.abs(scaled))))
        mean = primal if prev is None else 0.3 * primal + 0.7 * prev[here, :]
        mean_ref[here, :] = mean
        for s, p in enumerate(three_parts(mean)):
            parts_scr[pl.ds(group * 64 + s, 4, stride=8), :] = p[:4]
            parts_scr[pl.ds(group * 64 + 35 + s, 4, stride=8), :] = p[4:]
        for q in range(4):
            at = group * 64 + q * 8
            lhs = [parts_scr[at : at + 8, :], parts_scr[at + 32 : at + 40, :]]
            out = lax.dot_general(
                jnp.concatenate(lhs, axis=1).astype(bf16),
                inc_pair(group, q),
                (((1,), (1,)), ((), ())),
                preferred_element_type=f32,
            )
            for row, t in ((0, group * 8 + q), (3, group * 8 + q + 4)):
                part = out[row : row + 1] + out[row + 1 : row + 2] + out[row + 2 : row + 3]
                for k in range(K):
                    cover_ref[pl.ds(ids_ref[k, t], 1), :] += part[:, k * BLK : (k + 1) * BLK]
    soft_ref[...] = soft_sum


def first_kernel(
    ids_hbm, inc_hbm, cost_hbm, mult_hbm, inc_ref, mean_ref, soft_ref, cover_ref, sum_ref,
    ids, raw, cost, mult, rows_scr, parts_scr, sems,
):
    tiles = cost.shape[0]
    small = [
        pltpu.make_async_copy(src, dst, sems.at[tiles + i])
        for i, (src, dst) in enumerate(((ids_hbm, ids), (mult_hbm, mult), (cost_hbm, cost)))
    ]
    large = [pltpu.make_async_copy(inc_hbm.at[t], raw.at[t], sems.at[t]) for t in range(tiles)]
    for copy in small:
        copy.start()
    for group in range(0, tiles, 8):
        for q in range(4):
            large[group + q].start()
            large[group + q + 4].start()
    for copy in small:
        copy.wait()
    seen = set()

    def inc_pair(group, q):
        pair = group * 4 + q
        if pair not in seen:
            seen.add(pair)
            for side in range(2):
                t = group * 8 + side * 4 + q
                large[t].wait()
                inc_ref[pair, :, side * TILE : (side + 1) * TILE] = (
                    raw[t].reshape(K * BLK, TILE).astype(f32).astype(inc_ref.dtype)
                )
        return inc_ref[pair]

    column_step(mult, ids, cost, inc_pair, None, rows_scr, parts_scr, mean_ref, soft_ref, cover_ref)
    sum_ref[...] = total_of(mult[...])


def total_of(v):
    n = v.shape[0] // 8
    v = v.reshape(n, 8, BLK)
    chains = [v[i] for i in range(4)]
    for i in range(4, n):
        chains[i % 4] = chains[i % 4] + v[i]
    return (chains[0] + chains[1]) + (chains[2] + chains[3])


def row_step(own_ref, other_ref, mult_ref, sum_ref, upper_ref, new_ref):
    me = lax.axis_index("c")
    half = mult_ref.shape[0] // 2
    slopes, soft, norm = [], sum_ref[...], 0.0
    for ref in (own_ref, other_ref):
        slope = 1.0 - ref[:, : SLOT - 8, :].reshape(half, BLK)
        slopes.append(slope)
        norm = norm + total_of(slope * slope)
        soft = soft + total_of(ref[:, SLOT - 8 :, :].reshape(half // 2, BLK))
    value = jnp.sum(soft, keepdims=True)
    size = (upper_ref[0] - value) / (jnp.sum(norm, keepdims=True) + 1e-06)
    for slope, core in zip(slopes, (me, 1 - me)):
        at = pl.ds(pl.multiple_of(core * half, half), half)
        new_ref[at, :] = jnp.maximum(0.0, mult_ref[at, :] + size * slope)


def next_kernel(
    own_ref, other_ref, mult_ref, sum_ref, upper_ref, ids_ref, inc_ref, cost_ref, prev_ref,
    new_ref, mean_ref, soft_ref, cover_ref, total_ref, rows_scr, parts_scr,
):
    row_step(own_ref, other_ref, mult_ref, sum_ref, upper_ref, new_ref)
    column_step(
        new_ref, ids_ref, cost_ref, lambda group, q: inc_ref[group * 4 + q],
        prev_ref, rows_scr, parts_scr, mean_ref, soft_ref, cover_ref,
    )
    total_ref[...] = total_of(new_ref[...])


def last_kernel(own_ref, other_ref, mult_ref, sum_ref, upper_ref, mean_ref, new_ref, out_ref):
    out_ref[...] = mean_ref[...]
    row_step(own_ref, other_ref, mult_ref, sum_ref, upper_ref, new_ref)


def owner_kernel(in_ref, soft_ref, out_ref):
    total = in_ref[0]
    for i in range(1, in_ref.shape[0]):
        total += in_ref[i]
    for i in range(out_ref.shape[0]):
        out_ref[i, : SLOT - 8] = total
        out_ref[i, SLOT - 8 :] = soft_ref[...]


def spread_kernel(in_ref, out_ref):
    total = in_ref[0]
    for i in range(1, in_ref.shape[0]):
        total += in_ref[i]
    for i in range(out_ref.shape[0]):
        out_ref[i] = total


def call(kernel, name, out, specs, scratch=(), mib=8):
    return pl.pallas_call(
        kernel,
        out_shape=out,
        in_specs=specs,
        out_specs=jax.tree.map(lambda _: VMEM, out),
        scratch_shapes=scratch,
        compiler_params=pltpu.CompilerParams(vmem_limit_bytes=mib << 20),
        name=name,
    )


def local(block_ids, incidence, costs, start_mult, upper):
    tiles, rows = block_ids.shape[0], start_mult.shape[0]
    sds = jax.ShapeDtypeStruct
    ids = block_ids.T
    tile_sums, multipliers, columns = sds((8, TILE), f32), sds((rows, BLK), f32), sds((tiles, TILE), f32)
    outs = (columns, tile_sums, multipliers, tile_sums)
    scratch = [pltpu.VMEM((tiles * K, BLK), f32), pltpu.VMEM((tiles * 8, TILE), f32)]
    inc, mean, soft, cover, total = call(
        first_kernel,
        "first",
        (sds((tiles // 2, K * BLK, 2 * TILE), INC), *outs),
        [HBM] * 4,
        [
            pltpu.SMEM((K, tiles), jnp.int32),
            pltpu.VMEM((tiles, K, BLK, TILE), jnp.int32),
            pltpu.VMEM((tiles, TILE), jnp.int32),
            pltpu.VMEM((rows, BLK), f32),
            *scratch,
            pltpu.SemaphoreType.DMA((tiles + 3,)),
        ],
        mib=16,
    )(*(pltpu.with_memory_space_constraint(a, pltpu.HBM) for a in (ids, incidence, costs, start_mult)))
    mult = start_mult
    for step in range(ITERS):
        there = lax.all_to_all(cover.reshape(C * X * Y, SLOT - 8, BLK), OWNERS, 0, 0, tiled=True)
        there = call(owner_kernel, "owner", sds((Z, SLOT, BLK), f32), [VMEM] * 2)(there, soft)
        there = lax.all_to_all(there, "z", 0, 0, tiled=True)
        there = call(spread_kernel, "spread", sds((X * Y, SLOT, BLK), f32), [VMEM])(there)
        own = lax.all_to_all(there, NEAR, 0, 0, tiled=True)
        other = lax.ppermute(own, "c", [(0, 1), (1, 0)])
        rows_in = (own, other, mult, total, upper)
        if step < ITERS - 1:
            mult, mean, soft, cover, total = call(
                next_kernel,
                "next",
                (multipliers, *outs),
                [VMEM] * 4 + [SMEM] * 2 + [VMEM] * 3,
                scratch,
            )(*rows_in, ids, inc, costs, mean)
    return call(last_kernel, "last", (multipliers, columns), [VMEM] * 4 + [SMEM, VMEM])(*rows_in, mean)


def solution(mesh):
    split = Mesh(mesh.devices.reshape(X, C, Y, Z), SPLIT)
    return jax.shard_map(
        local,
        mesh=split,
        in_specs=(
            P(SPLIT, None),
            P(SPLIT, None, None, None),
            P(SPLIT, None),
            P(),
            P(),
        ),
        out_specs=(P(), P(SPLIT, None)),
        check_vma=False,
    )
```

```python
import jax
import jax.numpy as jnp
from jax import lax
from jax.experimental import pallas as pl
from jax.experimental.pallas import tpu as pltpu
from jax.sharding import Mesh
from jax.sharding import PartitionSpec as P

BLK = 128
TILE = 128
K = 4
ITERS = 3
X, C, Y, Z = 4, 2, 4, 8
SPLIT = ("x", "c", "y", "z")
OWNERS = ("c", "x", "y")
NEAR = ("x", "y")
SLOT = 24

f32, bf16 = jnp.float32, jnp.bfloat16
INC = jnp.float8_e4m3fn
VMEM = pl.BlockSpec(memory_space=pltpu.VMEM)
SMEM = pl.BlockSpec(memory_space=pltpu.SMEM)
HBM = pl.BlockSpec(memory_space=pltpu.HBM)


def three_parts(v):
    high = v.astype(bf16).astype(f32)
    rest = v - high
    middle = rest.astype(bf16).astype(f32)
    return high, middle, rest - middle


def column_step(mult_ref, ids_ref, cost_ref, inc_pair, prev, rows_scr, parts_scr, mean_ref, soft_ref, cover_ref):
    tiles = cost_ref.shape[0]
    for t in range(tiles):
        for k in range(K):
            at = (t // 8 * K + k) * 8 + t % 8
            rows_scr[at : at + 1, :] = mult_ref[pl.ds(ids_ref[k, t], 1), :]
    parts_scr[...] = jnp.zeros_like(parts_scr)
    cover_ref[...] = jnp.zeros_like(cover_ref)
    line = lax.broadcasted_iota(jnp.int32, (8, BLK), 0)
    none = jnp.zeros((8, BLK), f32)
    soft_sum = none
    for group in range(tiles // 8):
        parts = [
            three_parts(rows_scr[(group * K + k) * 8 : (group * K + k + 1) * 8, :]) for k in range(K)
        ]
        acc = jnp.zeros((32, 2 * TILE), f32)
        for q in range(4):
            keep = line % 4 == q
            lhs = [
                jnp.concatenate([jnp.where(keep, p, 0.0) for p in parts[k]] + [none], axis=0)
                for k in range(K)
            ]
            lhs = jnp.concatenate(lhs, axis=1).astype(bf16)
            acc += jnp.dot(lhs, inc_pair(group, q), preferred_element_type=f32)
        here = slice(group * 8, group * 8 + 8)
        both = acc[:8] + acc[8:16] + acc[16:24]
        priced = jnp.where(line < 4, both[:, :TILE], both[:, TILE:])
        reduced = cost_ref[here, :].astype(f32) - priced
        scaled = reduced / 8.0
        primal = 1.0 / (1.0 + jnp.exp(scaled))
        soft_sum += -8.0 * (jnp.maximum(-scaled, 0.0) + jnp.log1p(jnp.exp(-jnp.abs(scaled))))
        mean = primal if prev is None else 0.3 * primal + 0.7 * prev[here, :]
        mean_ref[here, :] = mean
        for s, p in enumerate(three_parts(mean)):
            parts_scr[pl.ds(group * 64 + s, 4, stride=8), :] = p[:4]
            parts_scr[pl.ds(group * 64 + 35 + s, 4, stride=8), :] = p[4:]
        for q in range(4):
            at = group * 64 + q * 8
            lhs = [parts_scr[at : at + 8, :], parts_scr[at + 32 : at + 40, :]]
            out = lax.dot_general(
                jnp.concatenate(lhs, axis=1).astype(bf16),
                inc_pair(group, q),
                (((1,), (1,)), ((), ())),
                preferred_element_type=f32,
            )
            for row, t in ((0, group * 8 + q), (3, group * 8 + q + 4)):
                part = out[row : row + 1] + out[row + 1 : row + 2] + out[row + 2 : row + 3]
                for k in range(K):
                    cover_ref[pl.ds(ids_ref[k, t], 1), :] += part[:, k * BLK : (k + 1) * BLK]
    soft_ref[...] = soft_sum


def first_kernel(
    ids_hbm, inc_hbm, cost_hbm, mult_hbm, inc_ref, mean_ref, soft_ref, cover_ref, sum_ref,
    ids, raw, cost, mult, rows_scr, parts_scr, sems,
):
    tiles = cost.shape[0]
    small = [
        pltpu.make_async_copy(src, dst, sems.at[tiles + i])
        for i, (src, dst) in enumerate(((ids_hbm, ids), (mult_hbm, mult), (cost_hbm, cost)))
    ]
    large = [pltpu.make_async_copy(inc_hbm.at[t], raw.at[t], sems.at[t]) for t in range(tiles)]
    for copy in small:
        copy.start()
    for group in range(0, tiles, 8):
        for q in range(4):
            large[group + q].start()
            large[group + q + 4].start()
    for copy in small:
        copy.wait()
    seen = set()

    def inc_pair(group, q):
        pair = group * 4 + q
        if pair not in seen:
            seen.add(pair)
            for side in range(2):
                t = group * 8 + side * 4 + q
                large[t].wait()
                inc_ref[pair, :, side * TILE : (side + 1) * TILE] = (
                    raw[t].reshape(K * BLK, TILE).astype(f32).astype(inc_ref.dtype)
                )
        return inc_ref[pair]

    column_step(mult, ids, cost, inc_pair, None, rows_scr, parts_scr, mean_ref, soft_ref, cover_ref)
    sum_ref[...] = total_of(mult[...])


def total_of(v):
    n = v.shape[0] // 8
    v = v.reshape(n, 8, BLK)
    chains = [v[i] for i in range(4)]
    for i in range(4, n):
        chains[i % 4] = chains[i % 4] + v[i]
    return (chains[0] + chains[1]) + (chains[2] + chains[3])


def row_step(own_ref, other_ref, mult_ref, sum_ref, upper_ref, new_ref):
    me = lax.axis_index("c")
    half = mult_ref.shape[0] // 2
    slopes, soft, norm = [], sum_ref[...], 0.0
    for ref in (own_ref, other_ref):
        slope = 1.0 - ref[:, : SLOT - 8, :].reshape(half, BLK)
        slopes.append(slope)
        norm = norm + total_of(slope * slope)
        soft = soft + total_of(ref[:, SLOT - 8 :, :].reshape(half // 2, BLK))
    value = jnp.sum(soft, keepdims=True)
    size = (upper_ref[0] - value) / (jnp.sum(norm, keepdims=True) + 1e-06)
    for slope, core in zip(slopes, (me, 1 - me)):
        at = pl.ds(pl.multiple_of(core * half, half), half)
        new_ref[at, :] = jnp.maximum(0.0, mult_ref[at, :] + size * slope)


def next_kernel(
    own_ref, other_ref, mult_ref, sum_ref, upper_ref, ids_ref, inc_ref, cost_ref, prev_ref,
    new_ref, mean_ref, soft_ref, cover_ref, total_ref, rows_scr, parts_scr,
):
    row_step(own_ref, other_ref, mult_ref, sum_ref, upper_ref, new_ref)
    column_step(
        new_ref, ids_ref, cost_ref, lambda group, q: inc_ref[group * 4 + q],
        prev_ref, rows_scr, parts_scr, mean_ref, soft_ref, cover_ref,
    )
    total_ref[...] = total_of(new_ref[...])


def last_kernel(own_ref, other_ref, mult_ref, sum_ref, upper_ref, mean_ref, new_ref, out_ref):
    out_ref[...] = mean_ref[...]
    row_step(own_ref, other_ref, mult_ref, sum_ref, upper_ref, new_ref)


def owner_kernel(in_ref, soft_ref, out_ref):
    total = in_ref[0]
    for i in range(1, in_ref.shape[0]):
        total += in_ref[i]
    for i in range(out_ref.shape[0]):
        out_ref[i, : SLOT - 8] = total
        out_ref[i, SLOT - 8 :] = soft_ref[...]


def spread_kernel(in_ref, out_ref):
    total = in_ref[0]
    for i in range(1, in_ref.shape[0]):
        total += in_ref[i]
    for i in range(out_ref.shape[0]):
        out_ref[i] = total


def call(kernel, name, out, specs, scratch=(), mib=8):
    return pl.pallas_call(
        kernel,
        out_shape=out,
        in_specs=specs,
        out_specs=jax.tree.map(lambda _: VMEM, out),
        scratch_shapes=scratch,
        compiler_params=pltpu.CompilerParams(vmem_limit_bytes=mib << 20),
        name=name,
    )


def local(block_ids, incidence, costs, start_mult, upper):
    tiles, rows = block_ids.shape[0], start_mult.shape[0]
    sds = jax.ShapeDtypeStruct
    ids = block_ids.T
    tile_sums, multipliers, columns = sds((8, TILE), f32), sds((rows, BLK), f32), sds((tiles, TILE), f32)
    outs = (columns, tile_sums, multipliers, tile_sums)
    scratch = [pltpu.VMEM((tiles * K, BLK), f32), pltpu.VMEM((tiles * 8, TILE), f32)]
    inc, mean, soft, cover, total = call(
        first_kernel,
        "first",
        (sds((tiles // 2, K * BLK, 2 * TILE), INC), *outs),
        [HBM] * 4,
        [
            pltpu.SMEM((K, tiles), jnp.int32),
            pltpu.VMEM((tiles, K, BLK, TILE), jnp.int32),
            pltpu.VMEM((tiles, TILE), jnp.int32),
            pltpu.VMEM((rows, BLK), f32),
            *scratch,
            pltpu.SemaphoreType.DMA((tiles + 3,)),
        ],
        mib=16,
    )(*(pltpu.with_memory_space_constraint(a, pltpu.HBM) for a in (ids, incidence, costs, start_mult)))
    mult = start_mult
    for step in range(ITERS):
        there = lax.all_to_all(cover.reshape(C * X * Y, SLOT - 8, BLK), OWNERS, 0, 0, tiled=True)
        there = call(owner_kernel, "owner", sds((Z, SLOT, BLK), f32), [VMEM] * 2)(there, soft)
        there = lax.all_to_all(there, "z", 0, 0, tiled=True)
        there = call(spread_kernel, "spread", sds((X * Y, SLOT, BLK), f32), [VMEM])(there)
        own = lax.all_to_all(there, NEAR, 0, 0, tiled=True)
        other = lax.ppermute(own, "c", [(0, 1), (1, 0)])
        rows_in = (own, other, mult, total, upper)
        if step < ITERS - 1:
            mult, mean, soft, cover, total = call(
                next_kernel,
                "next",
                (multipliers, *outs),
                [VMEM] * 4 + [SMEM] * 2 + [VMEM] * 3,
                scratch,
            )(*rows_in, ids, inc, costs, mean)
    return call(last_kernel, "last", (multipliers, columns), [VMEM] * 4 + [SMEM, VMEM])(*rows_in, mean)


def solution(mesh):
    split = Mesh(mesh.devices.reshape(X, C, Y, Z), SPLIT)
    return jax.shard_map(
        local,
        mesh=split,
        in_specs=(
            P(SPLIT, None),
            P(SPLIT, None, None, None),
            P(SPLIT, None),
            P(),
            P(),
        ),
        out_specs=(P(), P(SPLIT, None)),
        check_vma=False,
    )
```

```python
import jax
import jax.numpy as jnp
from jax import lax
from jax.experimental import pallas as pl
from jax.experimental.pallas import tpu as pltpu
from jax.sharding import Mesh
from jax.sharding import PartitionSpec as P

BLK = 128
TILE = 128
K = 4
ITERS = 3
X, C, Y, Z = 4, 2, 4, 8
NEAR, FAR = X * Y, Z
OWN = 16
SLOT = OWN + 8
PLANE_ORDER = (
    (1, 2), (2, 2), (0, 2), (0, 1), (3, 3), (2, 3), (0, 3), (0, 0),
    (3, 2), (1, 0), (1, 3), (3, 1), (2, 1), (1, 1), (2, 0), (3, 0),
)
LINE_ORDER = (0, 2, 4, 6, 7, 1, 3, 5)


def device(x, c, y, z):
    return ((x * C + c) * Y + y) * Z + z


PLANES = [[device(x, c, y, z) for x, y in PLANE_ORDER] for c in range(C) for z in range(Z)]
LINES = [
    [device(x, c, y, z) for z in LINE_ORDER] for x in range(X) for c in range(C) for y in range(Y)
]
SWAP = [
    (device(x, c, y, z), device(x, 1 - c, y, z))
    for x in range(X)
    for c in range(C)
    for y in range(Y)
    for z in range(Z)
]

f32, bf16 = jnp.float32, jnp.bfloat16
INC = jnp.float8_e4m3fn
VMEM = pl.BlockSpec(memory_space=pltpu.VMEM)
SMEM = pl.BlockSpec(memory_space=pltpu.SMEM)
ANY = pl.BlockSpec(memory_space=pl.ANY)
HBM = pl.BlockSpec(memory_space=pltpu.HBM)


def my_core():
    return (lax.axis_index("d") >> 5) & 1


def three_parts(v):
    high = v.astype(bf16).astype(f32)
    rest = v - high
    middle = rest.astype(bf16).astype(f32)
    return high, middle, rest - middle


def column_step(mult_ref, ids_ref, cost_ref, inc_pair, prev, rows_scr, parts_scr, cover_scr, mean_ref, soft_ref, mine_ref, send_ref):
    tiles = cost_ref.shape[0]
    for t in range(tiles):
        for k in range(K):
            at = (t // 8 * K + k) * 8 + t % 8
            rows_scr[at : at + 1, :] = mult_ref[pl.ds(ids_ref[k, t], 1), :]
    parts_scr[...] = jnp.zeros_like(parts_scr)
    cover_scr[...] = jnp.zeros_like(cover_scr)
    half = mine_ref.shape[0]
    turn = my_core() * half
    line = lax.broadcasted_iota(jnp.int32, (8, BLK), 0)
    none = jnp.zeros((8, BLK), f32)
    soft_sum = none
    for group in range(tiles // 8):
        parts = [
            three_parts(rows_scr[(group * K + k) * 8 : (group * K + k + 1) * 8, :]) for k in range(K)
        ]
        acc = jnp.zeros((32, 2 * TILE), f32)
        for q in range(4):
            keep = line % 4 == q
            lhs = [
                jnp.concatenate([jnp.where(keep, p, 0.0) for p in parts[k]] + [none], axis=0)
                for k in range(K)
            ]
            lhs = jnp.concatenate(lhs, axis=1).astype(bf16)
            acc += jnp.dot(lhs, inc_pair(group, q), preferred_element_type=f32)
        here = slice(group * 8, group * 8 + 8)
        both = acc[:8] + acc[8:16] + acc[16:24]
        priced = jnp.where(line < 4, both[:, :TILE], both[:, TILE:])
        reduced = cost_ref[here, :].astype(f32) - priced
        scaled = reduced / 8.0
        primal = 1.0 / (1.0 + jnp.exp(scaled))
        soft_sum += -8.0 * (jnp.maximum(-scaled, 0.0) + jnp.log1p(jnp.exp(-jnp.abs(scaled))))
        mean = primal if prev is None else 0.3 * primal + 0.7 * prev[here, :]
        mean_ref[here, :] = mean
        for s, p in enumerate(three_parts(mean)):
            parts_scr[pl.ds(group * 64 + s, 4, stride=8), :] = p[:4]
            parts_scr[pl.ds(group * 64 + 35 + s, 4, stride=8), :] = p[4:]
        for q in range(4):
            at = group * 64 + q * 8
            lhs = [parts_scr[at : at + 8, :], parts_scr[at + 32 : at + 40, :]]
            out = lax.dot_general(
                jnp.concatenate(lhs, axis=1).astype(bf16),
                inc_pair(group, q),
                (((1,), (1,)), ((), ())),
                preferred_element_type=f32,
            )
            for row, t in ((0, group * 8 + q), (3, group * 8 + q + 4)):
                part = out[row : row + 1] + out[row + 1 : row + 2] + out[row + 2 : row + 3]
                for k in range(K):
                    cover_scr[pl.ds(ids_ref[k, t] ^ turn, 1), :] += part[:, k * BLK : (k + 1) * BLK]
    soft_ref[...] = soft_sum
    mine_ref[...] = cover_scr[:half, :]
    send_ref[:half, :] = cover_scr[half:, :]
    send_ref[half:, :] = soft_sum


def first_kernel(
    ids_hbm, inc_hbm, cost_hbm, mult_hbm, inc_ref, mean_ref, soft_ref, mine_ref, send_ref, sum_ref,
    ids, raw, cost, mult, rows_scr, parts_scr, cover_scr, sems,
):
    tiles = cost.shape[0]
    small = [
        pltpu.make_async_copy(src, dst, sems.at[tiles + i])
        for i, (src, dst) in enumerate(((ids_hbm, ids), (mult_hbm, mult), (cost_hbm, cost)))
    ]
    large = [pltpu.make_async_copy(inc_hbm.at[t], raw.at[t], sems.at[t]) for t in range(tiles)]
    for copy in small:
        copy.start()
    for group in range(0, tiles, 8):
        for q in range(4):
            large[group + q].start()
            large[group + q + 4].start()
    for copy in small:
        copy.wait()
    seen = set()

    def inc_pair(group, q):
        pair = group * 4 + q
        if pair not in seen:
            seen.add(pair)
            for side in range(2):
                t = group * 8 + side * 4 + q
                large[t].wait()
                inc_ref[pair, :, side * TILE : (side + 1) * TILE] = (
                    raw[t].reshape(K * BLK, TILE).astype(f32).astype(inc_ref.dtype)
                )
        return inc_ref[pair]

    column_step(
        mult, ids, cost, inc_pair, None,
        rows_scr, parts_scr, cover_scr, mean_ref, soft_ref, mine_ref, send_ref,
    )
    sum_ref[...] = total_of(mult[...])


def total_of(v):
    n = v.shape[0] // 8
    v = v.reshape(n, 8, BLK)
    chains = [v[i] for i in range(4)]
    for i in range(4, n):
        chains[i % 4] = chains[i % 4] + v[i]
    return (chains[0] + chains[1]) + (chains[2] + chains[3])


def row_step(own_ref, other_ref, soft_ref, mult_ref, sum_ref, upper_ref, new_ref):
    me = my_core()
    half = mult_ref.shape[0] // 2
    slopes = [1.0 - ref[...].reshape(half, BLK) for ref in (own_ref, other_ref)]
    norm = total_of(slopes[0] * slopes[0]) + total_of(slopes[1] * slopes[1])
    value = jnp.sum(soft_ref[...] + sum_ref[...], keepdims=True)
    size = (upper_ref[0] - value) / (jnp.sum(norm, keepdims=True) + 1e-06)
    for slope, core in zip(slopes, (me, 1 - me)):
        at = pl.ds(pl.multiple_of(core * half, half), half)
        new_ref[at, :] = jnp.maximum(0.0, mult_ref[at, :] + size * slope)


def next_kernel(
    own_ref, other_ref, all_ref, mult_ref, sum_ref, upper_ref, ids_any, inc_ref, cost_ref, prev_ref,
    new_ref, mean_ref, soft_ref, mine_ref, send_ref, total_ref,
    ids, rows_scr, parts_scr, cover_scr, sem,
):
    copy = pltpu.make_async_copy(ids_any, ids, sem)
    copy.start()
    row_step(own_ref, other_ref, all_ref, mult_ref, sum_ref, upper_ref, new_ref)
    copy.wait()
    column_step(
        new_ref, ids, cost_ref, lambda group, q: inc_ref[group * 4 + q], prev_ref,
        rows_scr, parts_scr, cover_scr, mean_ref, soft_ref, mine_ref, send_ref,
    )
    total_ref[...] = total_of(new_ref[...])


def last_kernel(own_ref, other_ref, all_ref, mult_ref, sum_ref, upper_ref, mean_ref, new_ref, out_ref):
    out_ref[...] = mean_ref[...]
    row_step(own_ref, other_ref, all_ref, mult_ref, sum_ref, upper_ref, new_ref)


def pair_kernel(mine_ref, soft_ref, got_ref, out_ref):
    half = mine_ref.shape[0]
    out_ref[:, :OWN, :] = (mine_ref[...] + got_ref[:half, :]).reshape(NEAR, OWN, BLK)
    soft = soft_ref[...] + got_ref[half:, :]
    for i in range(NEAR):
        out_ref[i, OWN:, :] = soft


def sum_of(ref):
    parts = [ref[i] for i in range(ref.shape[0])]
    while len(parts) > 1:
        parts = [a + b for a, b in zip(parts[::2], parts[1::2])]
    return parts[0]


def owner_kernel(in_ref, out_ref):
    total = sum_of(in_ref)
    for i in range(FAR):
        out_ref[i] = total


def spread_kernel(in_ref, out_ref, soft_ref):
    total = sum_of(in_ref)
    for i in range(NEAR):
        out_ref[i] = total[:OWN]
    soft_ref[...] = total[OWN:]


def call(kernel, name, out, specs, scratch=(), mib=8):
    return pl.pallas_call(
        kernel,
        out_shape=out,
        in_specs=specs,
        out_specs=jax.tree.map(lambda _: VMEM, out),
        scratch_shapes=scratch,
        compiler_params=pltpu.CompilerParams(vmem_limit_bytes=mib << 20),
        name=name,
    )


def exchange(blocks, groups):
    return lax.all_to_all(blocks, "d", 0, 0, tiled=True, axis_index_groups=groups)


def local(block_ids, incidence, costs, start_mult, upper):
    tiles, rows = block_ids.shape[0], start_mult.shape[0]
    half = rows // 2
    ids = block_ids.T

    def floats(*shape):
        return jax.ShapeDtypeStruct((*shape, BLK), f32)

    outs = (floats(tiles), floats(8), floats(half), floats(half + 8), floats(8))
    scratch = [pltpu.VMEM((n, BLK), f32) for n in (tiles * K, tiles * 8, rows)]
    inc, mean, soft, mine, send, total = call(
        first_kernel,
        "first",
        (jax.ShapeDtypeStruct((tiles // 2, K * BLK, 2 * TILE), INC), *outs),
        [HBM] * 4,
        [
            pltpu.SMEM((K, tiles), jnp.int32),
            pltpu.VMEM((tiles, K, BLK, TILE), jnp.int32),
            pltpu.VMEM((tiles, TILE), jnp.int32),
            pltpu.VMEM((rows, BLK), f32),
            *scratch,
            pltpu.SemaphoreType.DMA((tiles + 3,)),
        ],
        mib=16,
    )(*(pltpu.with_memory_space_constraint(a, pltpu.HBM) for a in (ids, incidence, costs, start_mult)))
    mult = start_mult
    for step in range(ITERS):
        got = lax.ppermute(send, "d", SWAP)
        there = call(pair_kernel, "pair", floats(NEAR, SLOT), [VMEM] * 3)(mine, soft, got)
        there = exchange(there, PLANES)
        there = call(owner_kernel, "owner", floats(FAR, SLOT), [VMEM])(there)
        there = exchange(there, LINES)
        there, soft = call(spread_kernel, "spread", (floats(NEAR, OWN), floats(8)), [VMEM])(there)
        own = exchange(there, PLANES)
        other = lax.ppermute(own, "d", SWAP)
        rows_in = (own, other, soft, mult, total, upper)
        if step < ITERS - 1:
            mult, mean, soft, mine, send, total = call(
                next_kernel,
                "next",
                (floats(rows), *outs),
                [VMEM] * 5 + [SMEM, ANY] + [VMEM] * 3,
                [pltpu.SMEM((K, tiles), jnp.int32), *scratch, pltpu.SemaphoreType.DMA],
            )(*rows_in, ids, inc, costs, mean)
    return call(last_kernel, "last", (floats(rows), floats(tiles)), [VMEM] * 5 + [SMEM, VMEM])(*rows_in, mean)


def solution(mesh):
    return jax.shard_map(
        local,
        mesh=Mesh(mesh.devices.reshape(-1), ("d",)),
        in_specs=(
            P("d", None),
            P("d", None, None, None),
            P("d", None),
            P(),
            P(),
        ),
        out_specs=(P(), P("d", None)),
        check_vma=False,
    )
```

```python
import jax
import jax.numpy as jnp
from jax import lax
from jax.experimental import pallas as pl
from jax.experimental.pallas import tpu as pltpu
from jax.sharding import Mesh
from jax.sharding import PartitionSpec as P

BLK = 128
TILE = 128
K = 4
ITERS = 3
X, C, Y, Z = 4, 2, 4, 8
NEAR, FAR = X * C * Y, Z
OWN = 16
SLOT = OWN + 1
PLANE_ORDER = (
    (2, 1, 1), (1, 1, 2), (1, 0, 2), (0, 1, 0), (0, 1, 1), (1, 0, 1), (3, 1, 1), (0, 0, 1),
    (3, 1, 3), (1, 1, 1), (3, 1, 2), (2, 0, 3), (3, 0, 2), (3, 0, 0), (3, 0, 3), (1, 0, 0),
    (0, 1, 3), (3, 0, 1), (2, 1, 3), (0, 0, 0), (2, 0, 2), (3, 1, 0), (0, 0, 3), (2, 1, 2),
    (0, 1, 2), (2, 1, 0), (1, 1, 3), (2, 0, 0), (1, 1, 0), (0, 0, 2), (2, 0, 1), (1, 0, 3),
)
LINE_ORDER = (0, 2, 4, 6, 7, 1, 3, 5)


def device(x, c, y, z):
    return ((x * C + c) * Y + y) * Z + z


PLANES = [[device(x, c, y, z) for x, c, y in PLANE_ORDER] for z in range(Z)]
LINES = [
    [device(x, c, y, z) for z in LINE_ORDER] for x in range(X) for c in range(C) for y in range(Y)
]

f32, bf16 = jnp.float32, jnp.bfloat16
INC = jnp.float8_e4m3fn
VMEM = pl.BlockSpec(memory_space=pltpu.VMEM)
ANY = pl.BlockSpec(memory_space=pl.ANY)
HBM = pl.BlockSpec(memory_space=pltpu.HBM)


def three_parts(v):
    high = v.astype(bf16).astype(f32)
    rest = v - high
    middle = rest.astype(bf16).astype(f32)
    return high, middle, rest - middle


def column_step(mult_ref, ids_ref, cost_ref, inc_pair, prev, rows_scr, parts_scr, mean_ref, soft_ref, cover_ref):
    tiles = cost_ref.shape[0]
    for t in range(tiles):
        for k in range(K):
            at = (t // 8 * K + k) * 8 + t % 8
            rows_scr[at : at + 1, :] = mult_ref[pl.ds(ids_ref[k, t], 1), :]
    parts_scr[...] = jnp.zeros_like(parts_scr)
    cover_ref[...] = jnp.zeros_like(cover_ref)
    line = lax.broadcasted_iota(jnp.int32, (8, BLK), 0)
    none = jnp.zeros((8, BLK), f32)
    soft_sum = none
    for group in range(tiles // 8):
        parts = [
            three_parts(rows_scr[(group * K + k) * 8 : (group * K + k + 1) * 8, :]) for k in range(K)
        ]
        acc = jnp.zeros((32, 2 * TILE), f32)
        for q in range(4):
            keep = line % 4 == q
            lhs = [
                jnp.concatenate([jnp.where(keep, p, 0.0) for p in parts[k]] + [none], axis=0)
                for k in range(K)
            ]
            lhs = jnp.concatenate(lhs, axis=1).astype(bf16)
            acc += jnp.dot(lhs, inc_pair(group, q), preferred_element_type=f32)
        here = slice(group * 8, group * 8 + 8)
        both = acc[:8] + acc[8:16] + acc[16:24]
        priced = jnp.where(line < 4, both[:, :TILE], both[:, TILE:])
        reduced = cost_ref[here, :].astype(f32) - priced
        scaled = reduced / 8.0
        primal = 1.0 / (1.0 + jnp.exp(scaled))
        soft_sum += -8.0 * (jnp.maximum(-scaled, 0.0) + jnp.log1p(jnp.exp(-jnp.abs(scaled))))
        mean = primal if prev is None else 0.3 * primal + 0.7 * prev[here, :]
        mean_ref[here, :] = mean
        for s, p in enumerate(three_parts(mean)):
            parts_scr[pl.ds(group * 64 + s, 4, stride=8), :] = p[:4]
            parts_scr[pl.ds(group * 64 + 35 + s, 4, stride=8), :] = p[4:]
        for q in range(4):
            at = group * 64 + q * 8
            lhs = [parts_scr[at : at + 8, :], parts_scr[at + 32 : at + 40, :]]
            out = lax.dot_general(
                jnp.concatenate(lhs, axis=1).astype(bf16),
                inc_pair(group, q),
                (((1,), (1,)), ((), ())),
                preferred_element_type=f32,
            )
            for row, t in ((0, group * 8 + q), (3, group * 8 + q + 4)):
                part = out[row : row + 1] + out[row + 1 : row + 2] + out[row + 2 : row + 3]
                for k in range(K):
                    cover_ref[pl.ds(ids_ref[k, t], 1), :] += part[:, k * BLK : (k + 1) * BLK]
    soft_ref[...] = soft_sum


def first_kernel(
    ids_hbm, inc_hbm, cost_hbm, mult_hbm, upper,
    inc_ref, mean_ref, soft_ref, cover_ref, sum_ref, upper_ref,
    ids, raw, cost, mult, rows_scr, parts_scr, sems,
):
    tiles = cost.shape[0]
    small = [
        pltpu.make_async_copy(src, dst, sems.at[tiles + i])
        for i, (src, dst) in enumerate(((ids_hbm, ids), (mult_hbm, mult), (cost_hbm, cost)))
    ]
    large = [pltpu.make_async_copy(inc_hbm.at[t], raw.at[t], sems.at[t]) for t in range(tiles)]
    for copy in small:
        copy.start()
    for group in range(0, tiles, 8):
        for q in range(4):
            large[group + q].start()
            large[group + q + 4].start()
    for copy in small:
        copy.wait()
    seen = set()

    def inc_pair(group, q):
        pair = group * 4 + q
        if pair not in seen:
            seen.add(pair)
            for side in range(2):
                t = group * 8 + side * 4 + q
                large[t].wait()
                inc_ref[pair, :, side * TILE : (side + 1) * TILE] = (
                    raw[t].reshape(K * BLK, TILE).astype(f32).astype(inc_ref.dtype)
                )
        return inc_ref[pair]

    column_step(mult, ids, cost, inc_pair, None, rows_scr, parts_scr, mean_ref, soft_ref, cover_ref)
    sum_ref[...] = total_of(mult[...])
    upper_ref[...] = jnp.full(upper_ref.shape, upper[0], f32)


def total_of(v):
    n = v.shape[0] // 8
    v = v.reshape(n, 8, BLK)
    chains = [v[i] for i in range(4)]
    for i in range(4, n):
        chains[i % 4] = chains[i % 4] + v[i]
    return (chains[0] + chains[1]) + (chains[2] + chains[3])


def row_step(gathered, mult_ref, sum_ref, upper_ref, new_ref):
    norm, soft = [], sum_ref[...]
    lines = []
    for i in range(NEAR):
        slope = 1.0 - gathered[i * SLOT : i * SLOT + OWN, :]
        norm.append(slope * slope)
        lines.append(gathered[i * SLOT + OWN : (i + 1) * SLOT, :])
    value = jnp.sum(soft, keepdims=True) + jnp.sum(tree_sum(lines), keepdims=True)
    size = (upper_ref[:1, :1] - value) / (jnp.sum(tree_sum(norm), keepdims=True) + 1e-06)
    for i in range(NEAR):
        slope = 1.0 - gathered[i * SLOT : i * SLOT + OWN, :]
        here = slice(i * OWN, (i + 1) * OWN)
        new_ref[here, :] = jnp.maximum(0.0, mult_ref[here, :] + size * slope)


def next_kernel(
    gathered, mult_ref, sum_ref, upper_ref, ids_any, inc_ref, cost_ref, prev_ref,
    new_ref, mean_ref, soft_ref, cover_ref, total_ref, ids, rows_scr, parts_scr, sem,
):
    copy = pltpu.make_async_copy(ids_any, ids, sem)
    copy.start()
    row_step(gathered, mult_ref, sum_ref, upper_ref, new_ref)
    copy.wait()
    column_step(
        new_ref, ids, cost_ref, lambda group, q: inc_ref[group * 4 + q],
        prev_ref, rows_scr, parts_scr, mean_ref, soft_ref, cover_ref,
    )
    total_ref[...] = total_of(new_ref[...])


def last_kernel(gathered, mult_ref, sum_ref, upper_ref, mean_ref, new_ref, out_ref):
    out_ref[...] = mean_ref[...]
    row_step(gathered, mult_ref, sum_ref, upper_ref, new_ref)


def tree_sum(parts):
    while len(parts) > 1:
        parts = [a + b for a, b in zip(parts[::2], parts[1::2])]
    return parts[0]


def owner_kernel(in_ref, soft_ref, out_ref):
    total = tree_sum([in_ref[i] for i in range(NEAR)])
    soft = jnp.sum(soft_ref[...], axis=0, keepdims=True)
    for i in range(FAR):
        out_ref[i * SLOT : i * SLOT + OWN, :] = total
        out_ref[i * SLOT + OWN : (i + 1) * SLOT, :] = soft


def spread_kernel(in_ref, out_ref):
    total = tree_sum([in_ref[i * SLOT : i * SLOT + OWN, :] for i in range(FAR)])
    soft = tree_sum([in_ref[i * SLOT + OWN : (i + 1) * SLOT, :] for i in range(FAR)])
    for i in range(NEAR):
        out_ref[i * SLOT : i * SLOT + OWN, :] = total
        out_ref[i * SLOT + OWN : (i + 1) * SLOT, :] = soft


def call(kernel, name, out, specs, scratch=(), mib=8):
    return pl.pallas_call(
        kernel,
        out_shape=out,
        in_specs=specs,
        out_specs=jax.tree.map(lambda _: VMEM, out),
        scratch_shapes=scratch,
        compiler_params=pltpu.CompilerParams(vmem_limit_bytes=mib << 20),
        name=name,
    )


def exchange(blocks, groups):
    shape = blocks.shape
    blocks = blocks.reshape(len(groups[0]), -1)
    return lax.all_to_all(blocks, "d", 0, 0, tiled=True, axis_index_groups=groups).reshape(shape)


def local(block_ids, incidence, costs, start_mult, upper):
    tiles, rows = block_ids.shape[0], start_mult.shape[0]
    ids = block_ids.T

    def floats(*shape):
        return jax.ShapeDtypeStruct((*shape, BLK), f32)

    outs = (floats(tiles), floats(8), floats(rows), floats(8))
    scratch = [pltpu.VMEM((n, BLK), f32) for n in (tiles * K, tiles * 8)]
    inc, mean, soft, cover, total, top = call(
        first_kernel,
        "first",
        (jax.ShapeDtypeStruct((tiles // 2, K * BLK, 2 * TILE), INC), *outs, floats(8)),
        [HBM] * 4 + [pl.BlockSpec(memory_space=pltpu.SMEM)],
        [
            pltpu.SMEM((K, tiles), jnp.int32),
            pltpu.VMEM((tiles, K, BLK, TILE), jnp.int32),
            pltpu.VMEM((tiles, TILE), jnp.int32),
            pltpu.VMEM((rows, BLK), f32),
            *scratch,
            pltpu.SemaphoreType.DMA((tiles + 3,)),
        ],
        mib=16,
    )(*(pltpu.with_memory_space_constraint(a, pltpu.HBM) for a in (ids, incidence, costs, start_mult)), upper)
    mult = start_mult
    for step in range(ITERS):
        there = lax.all_to_all(
            cover.reshape(NEAR, OWN, BLK), "d", 0, 0, tiled=True, axis_index_groups=PLANES
        )
        there = call(owner_kernel, "owner", floats(FAR * SLOT), [VMEM] * 2)(there, soft)
        there = exchange(there, LINES)
        there = call(spread_kernel, "spread", floats(NEAR * SLOT), [VMEM])(there)
        rows_in = (exchange(there, PLANES), mult, total, top)
        if step < ITERS - 1:
            mult, mean, soft, cover, total = call(
                next_kernel,
                "next",
                (floats(rows), *outs),
                [VMEM] * 4 + [ANY] + [VMEM] * 3,
                [pltpu.SMEM((K, tiles), jnp.int32), *scratch, pltpu.SemaphoreType.DMA],
            )(*rows_in, ids, inc, costs, mean)
    return call(last_kernel, "last", (floats(rows), floats(tiles)), [VMEM] * 5)(*rows_in, mean)


def solution(mesh):
    return jax.shard_map(
        local,
        mesh=Mesh(mesh.devices.reshape(-1), ("d",)),
        in_specs=(
            P("d", None),
            P("d", None, None, None),
            P("d", None),
            P(),
            P(),
        ),
        out_specs=(P(), P("d", None)),
        check_vma=False,
    )
```

```python
import jax
import jax.numpy as jnp
from jax import lax
from jax.experimental import pallas as pl
from jax.experimental.pallas import tpu as pltpu
from jax.sharding import Mesh
from jax.sharding import PartitionSpec as P

BLK = 128
TILE = 128
K = 4
ITERS = 3
X, C, Y, Z = 4, 2, 4, 8
NEAR, FAR = X * C * Y, Z
OWN = 16
SLOT = OWN + 1
PLANE_ORDER = (
    (1, 0, 2), (1, 1, 1), (3, 0, 3), (3, 1, 2), (2, 1, 1), (0, 1, 3), (0, 0, 1), (3, 0, 0),
    (2, 0, 3), (1, 0, 3), (0, 1, 2), (0, 1, 0), (1, 0, 0), (2, 1, 0), (3, 1, 1), (2, 0, 2),
    (1, 1, 2), (1, 0, 1), (3, 1, 3), (3, 0, 2), (2, 0, 1), (0, 0, 3), (0, 1, 1), (3, 1, 0),
    (2, 1, 3), (1, 1, 3), (0, 0, 2), (0, 0, 0), (1, 1, 0), (2, 0, 0), (3, 0, 1), (2, 1, 2),
)
LINE_ORDER = (6, 0, 3, 2, 5, 1, 4, 7)


def device(x, c, y, z):
    return ((x * C + c) * Y + y) * Z + z


PLANES = [[device(x, c ^ (z >> 2), y, z) for x, c, y in PLANE_ORDER] for z in range(Z)]
LINES = [
    [device(x, c ^ (z >> 2), y, z) for z in LINE_ORDER] for x in range(X) for c in range(C) for y in range(Y)
]

f32, bf16 = jnp.float32, jnp.bfloat16
INC = jnp.float8_e4m3fn
VMEM = pl.BlockSpec(memory_space=pltpu.VMEM)
ANY = pl.BlockSpec(memory_space=pl.ANY)
HBM = pl.BlockSpec(memory_space=pltpu.HBM)


def three_parts(v):
    high = v.astype(bf16).astype(f32)
    rest = v - high
    middle = rest.astype(bf16).astype(f32)
    return high, middle, rest - middle


def column_step(mult_ref, ids_ref, cost_ref, inc_pair, prev, rows_scr, parts_scr, mean_ref, soft_ref, cover_ref):
    tiles = cost_ref.shape[0]
    for t in range(tiles):
        for k in range(K):
            at = (t // 8 * K + k) * 8 + t % 8
            rows_scr[at : at + 1, :] = mult_ref[pl.ds(ids_ref[k, t], 1), :]
    parts_scr[...] = jnp.zeros_like(parts_scr)
    cover_ref[...] = jnp.zeros_like(cover_ref)
    line = lax.broadcasted_iota(jnp.int32, (8, BLK), 0)
    none = jnp.zeros((8, BLK), f32)
    soft_sum = none
    for group in range(tiles // 8):
        parts = [
            three_parts(rows_scr[(group * K + k) * 8 : (group * K + k + 1) * 8, :]) for k in range(K)
        ]
        acc = jnp.zeros((32, 2 * TILE), f32)
        for q in range(4):
            keep = line % 4 == q
            lhs = [
                jnp.concatenate([jnp.where(keep, p, 0.0) for p in parts[k]] + [none], axis=0)
                for k in range(K)
            ]
            lhs = jnp.concatenate(lhs, axis=1).astype(bf16)
            acc += jnp.dot(lhs, inc_pair(group, q), preferred_element_type=f32)
        here = slice(group * 8, group * 8 + 8)
        both = acc[:8] + acc[8:16] + acc[16:24]
        priced = jnp.where(line < 4, both[:, :TILE], both[:, TILE:])
        reduced = cost_ref[here, :].astype(f32) - priced
        scaled = reduced / 8.0
        primal = 1.0 / (1.0 + jnp.exp(scaled))
        soft_sum += -8.0 * (jnp.maximum(-scaled, 0.0) + jnp.log1p(jnp.exp(-jnp.abs(scaled))))
        mean = primal if prev is None else 0.3 * primal + 0.7 * prev[here, :]
        mean_ref[here, :] = mean
        for s, p in enumerate(three_parts(mean)):
            parts_scr[pl.ds(group * 64 + s, 4, stride=8), :] = p[:4]
            parts_scr[pl.ds(group * 64 + 35 + s, 4, stride=8), :] = p[4:]
        for q in range(4):
            at = group * 64 + q * 8
            lhs = [parts_scr[at : at + 8, :], parts_scr[at + 32 : at + 40, :]]
            out = lax.dot_general(
                jnp.concatenate(lhs, axis=1).astype(bf16),
                inc_pair(group, q),
                (((1,), (1,)), ((), ())),
                preferred_element_type=f32,
            )
            for row, t in ((0, group * 8 + q), (3, group * 8 + q + 4)):
                part = out[row : row + 1] + out[row + 1 : row + 2] + out[row + 2 : row + 3]
                for k in range(K):
                    cover_ref[pl.ds(ids_ref[k, t], 1), :] += part[:, k * BLK : (k + 1) * BLK]
    soft_ref[...] = soft_sum


def first_kernel(
    ids_hbm, inc_hbm, cost_hbm, mult_hbm, upper,
    inc_ref, mean_ref, soft_ref, cover_ref, sum_ref, upper_ref,
    ids, raw, cost, mult, rows_scr, parts_scr, sems,
):
    tiles = cost.shape[0]
    small = [
        pltpu.make_async_copy(src, dst, sems.at[tiles + i])
        for i, (src, dst) in enumerate(((ids_hbm, ids), (mult_hbm, mult), (cost_hbm, cost)))
    ]
    large = [pltpu.make_async_copy(inc_hbm.at[t], raw.at[t], sems.at[t]) for t in range(tiles)]
    for copy in small:
        copy.start()
    for group in range(0, tiles, 8):
        for q in range(4):
            large[group + q].start()
            large[group + q + 4].start()
    for copy in small:
        copy.wait()
    seen = set()

    def inc_pair(group, q):
        pair = group * 4 + q
        if pair not in seen:
            seen.add(pair)
            for side in range(2):
                t = group * 8 + side * 4 + q
                large[t].wait()
                inc_ref[pair, :, side * TILE : (side + 1) * TILE] = (
                    raw[t].reshape(K * BLK, TILE).astype(f32).astype(inc_ref.dtype)
                )
        return inc_ref[pair]

    column_step(mult, ids, cost, inc_pair, None, rows_scr, parts_scr, mean_ref, soft_ref, cover_ref)
    sum_ref[...] = total_of(mult[...])
    upper_ref[...] = jnp.full(upper_ref.shape, upper[0], f32)


def total_of(v):
    n = v.shape[0] // 8
    v = v.reshape(n, 8, BLK)
    chains = [v[i] for i in range(4)]
    for i in range(4, n):
        chains[i % 4] = chains[i % 4] + v[i]
    return (chains[0] + chains[1]) + (chains[2] + chains[3])


def row_step(gathered, mult_ref, sum_ref, upper_ref, new_ref):
    norm, soft = [], sum_ref[...]
    lines = []
    for i in range(NEAR):
        slope = 1.0 - gathered[i * SLOT : i * SLOT + OWN, :]
        norm.append(slope * slope)
        lines.append(gathered[i * SLOT + OWN : (i + 1) * SLOT, :])
    value = jnp.sum(soft, keepdims=True) + jnp.sum(tree_sum(lines), keepdims=True)
    size = (upper_ref[:1, :1] - value) / (jnp.sum(tree_sum(norm), keepdims=True) + 1e-06)
    for i in range(NEAR):
        slope = 1.0 - gathered[i * SLOT : i * SLOT + OWN, :]
        here = slice(i * OWN, (i + 1) * OWN)
        new_ref[here, :] = jnp.maximum(0.0, mult_ref[here, :] + size * slope)


def next_kernel(
    gathered, mult_ref, sum_ref, upper_ref, ids_any, inc_ref, cost_ref, prev_ref,
    new_ref, mean_ref, soft_ref, cover_ref, total_ref, ids, rows_scr, parts_scr, sem,
):
    copy = pltpu.make_async_copy(ids_any, ids, sem)
    copy.start()
    row_step(gathered, mult_ref, sum_ref, upper_ref, new_ref)
    copy.wait()
    column_step(
        new_ref, ids, cost_ref, lambda group, q: inc_ref[group * 4 + q],
        prev_ref, rows_scr, parts_scr, mean_ref, soft_ref, cover_ref,
    )
    total_ref[...] = total_of(new_ref[...])


def last_kernel(gathered, mult_ref, sum_ref, upper_ref, mean_ref, new_ref, out_ref):
    out_ref[...] = mean_ref[...]
    row_step(gathered, mult_ref, sum_ref, upper_ref, new_ref)


def tree_sum(parts):
    while len(parts) > 1:
        parts = [a + b for a, b in zip(parts[::2], parts[1::2])]
    return parts[0]


def owner_kernel(in_ref, soft_ref, out_ref):
    total = tree_sum([in_ref[i] for i in range(NEAR)])
    soft = jnp.sum(soft_ref[...], axis=0, keepdims=True)
    for i in range(FAR):
        out_ref[i * SLOT : i * SLOT + OWN, :] = total
        out_ref[i * SLOT + OWN : (i + 1) * SLOT, :] = soft


def spread_kernel(in_ref, out_ref):
    total = tree_sum([in_ref[i * SLOT : i * SLOT + OWN, :] for i in range(FAR)])
    soft = tree_sum([in_ref[i * SLOT + OWN : (i + 1) * SLOT, :] for i in range(FAR)])
    for i in range(NEAR):
        out_ref[i * SLOT : i * SLOT + OWN, :] = total
        out_ref[i * SLOT + OWN : (i + 1) * SLOT, :] = soft


def call(kernel, name, out, specs, scratch=(), mib=8):
    return pl.pallas_call(
        kernel,
        out_shape=out,
        in_specs=specs,
        out_specs=jax.tree.map(lambda _: VMEM, out),
        scratch_shapes=scratch,
        compiler_params=pltpu.CompilerParams(vmem_limit_bytes=mib << 20),
        name=name,
    )


def exchange(blocks, groups):
    shape = blocks.shape
    blocks = blocks.reshape(len(groups[0]), -1)
    return lax.all_to_all(blocks, "d", 0, 0, tiled=True, axis_index_groups=groups).reshape(shape)


def local(block_ids, incidence, costs, start_mult, upper):
    tiles, rows = block_ids.shape[0], start_mult.shape[0]
    ids = block_ids.T

    def floats(*shape):
        return jax.ShapeDtypeStruct((*shape, BLK), f32)

    outs = (floats(tiles), floats(8), floats(rows), floats(8))
    scratch = [pltpu.VMEM((n, BLK), f32) for n in (tiles * K, tiles * 8)]
    inc, mean, soft, cover, total, top = call(
        first_kernel,
        "first",
        (jax.ShapeDtypeStruct((tiles // 2, K * BLK, 2 * TILE), INC), *outs, floats(8)),
        [HBM] * 4 + [pl.BlockSpec(memory_space=pltpu.SMEM)],
        [
            pltpu.SMEM((K, tiles), jnp.int32),
            pltpu.VMEM((tiles, K, BLK, TILE), jnp.int32),
            pltpu.VMEM((tiles, TILE), jnp.int32),
            pltpu.VMEM((rows, BLK), f32),
            *scratch,
            pltpu.SemaphoreType.DMA((tiles + 3,)),
        ],
        mib=16,
    )(*(pltpu.with_memory_space_constraint(a, pltpu.HBM) for a in (ids, incidence, costs, start_mult)), upper)
    mult = start_mult
    for step in range(ITERS):
        there = lax.all_to_all(
            cover.reshape(NEAR, OWN, BLK), "d", 0, 0, tiled=True, axis_index_groups=PLANES
        )
        there = call(owner_kernel, "owner", floats(FAR * SLOT), [VMEM] * 2)(there, soft)
        there = exchange(there, LINES)
        there = call(spread_kernel, "spread", floats(NEAR * SLOT), [VMEM])(there)
        rows_in = (exchange(there, PLANES), mult, total, top)
        if step < ITERS - 1:
            mult, mean, soft, cover, total = call(
                next_kernel,
                "next",
                (floats(rows), *outs),
                [VMEM] * 4 + [ANY] + [VMEM] * 3,
                [pltpu.SMEM((K, tiles), jnp.int32), *scratch, pltpu.SemaphoreType.DMA],
            )(*rows_in, ids, inc, costs, mean)
    return call(last_kernel, "last", (floats(rows), floats(tiles)), [VMEM] * 5)(*rows_in, mean)


def solution(mesh):
    return jax.shard_map(
        local,
        mesh=Mesh(mesh.devices.reshape(-1), ("d",)),
        in_specs=(
            P("d", None),
            P("d", None, None, None),
            P("d", None),
            P(),
            P(),
        ),
        out_specs=(P(), P("d", None)),
        check_vma=False,
    )
```

```python
import jax
import jax.numpy as jnp
from jax import lax
from jax.experimental import pallas as pl
from jax.experimental.pallas import tpu as pltpu
from jax.sharding import Mesh
from jax.sharding import PartitionSpec as P

BLK = 128
TILE = 128
K = 4
ITERS = 3
X, C, Y, Z = 4, 2, 4, 8
NEAR, FAR = X * C * Y, Z
OWN = 16
SLOT = OWN + 1
PLANE_ORDER = (
    (1, 0, 2), (1, 1, 1), (3, 0, 3), (3, 1, 2), (2, 1, 1), (0, 1, 3), (0, 0, 1), (3, 0, 0),
    (2, 0, 3), (1, 0, 3), (0, 1, 2), (0, 1, 0), (1, 0, 0), (2, 1, 0), (3, 1, 1), (2, 0, 2),
    (1, 1, 2), (1, 0, 1), (3, 1, 3), (3, 0, 2), (2, 0, 1), (0, 0, 3), (0, 1, 1), (3, 1, 0),
    (2, 1, 3), (1, 1, 3), (0, 0, 2), (0, 0, 0), (1, 1, 0), (2, 0, 0), (3, 0, 1), (2, 1, 2),
)
LINE_ORDER = (6, 0, 3, 2, 5, 1, 4, 7)


def device(x, c, y, z):
    return ((x * C + c) * Y + y) * Z + z


PLANES = [[device(x, c ^ ((z ^ z >> 2) & 1), y, z) for x, c, y in PLANE_ORDER] for z in range(Z)]
LINES = [
    [device(x, c ^ ((z ^ z >> 2) & 1), y, z) for z in LINE_ORDER] for x in range(X) for c in range(C) for y in range(Y)
]

f32, bf16 = jnp.float32, jnp.bfloat16
INC = jnp.float8_e4m3fn
VMEM = pl.BlockSpec(memory_space=pltpu.VMEM)
ANY = pl.BlockSpec(memory_space=pl.ANY)
HBM = pl.BlockSpec(memory_space=pltpu.HBM)


def three_parts(v):
    high = v.astype(bf16).astype(f32)
    rest = v - high
    middle = rest.astype(bf16).astype(f32)
    return high, middle, rest - middle


def column_step(mult_ref, ids_ref, cost_ref, inc_pair, prev, rows_scr, parts_scr, mean_ref, soft_ref, cover_ref):
    tiles = cost_ref.shape[0]
    for t in range(tiles):
        for k in range(K):
            at = (t // 8 * K + k) * 8 + t % 8
            rows_scr[at : at + 1, :] = mult_ref[pl.ds(ids_ref[k, t], 1), :]
    parts_scr[...] = jnp.zeros_like(parts_scr)
    cover_ref[...] = jnp.zeros_like(cover_ref)
    line = lax.broadcasted_iota(jnp.int32, (8, BLK), 0)
    none = jnp.zeros((8, BLK), f32)
    soft_sum = none
    for group in range(tiles // 8):
        parts = [
            three_parts(rows_scr[(group * K + k) * 8 : (group * K + k + 1) * 8, :]) for k in range(K)
        ]
        acc = jnp.zeros((32, 2 * TILE), f32)
        for q in range(4):
            keep = line % 4 == q
            lhs = [
                jnp.concatenate([jnp.where(keep, p, 0.0) for p in parts[k]] + [none], axis=0)
                for k in range(K)
            ]
            lhs = jnp.concatenate(lhs, axis=1).astype(bf16)
            acc += jnp.dot(lhs, inc_pair(group, q), preferred_element_type=f32)
        here = slice(group * 8, group * 8 + 8)
        both = acc[:8] + acc[8:16] + acc[16:24]
        priced = jnp.where(line < 4, both[:, :TILE], both[:, TILE:])
        reduced = cost_ref[here, :].astype(f32) - priced
        scaled = reduced / 8.0
        primal = 1.0 / (1.0 + jnp.exp(scaled))
        soft_sum += -8.0 * (jnp.maximum(-scaled, 0.0) + jnp.log1p(jnp.exp(-jnp.abs(scaled))))
        mean = primal if prev is None else 0.3 * primal + 0.7 * prev[here, :]
        mean_ref[here, :] = mean
        for s, p in enumerate(three_parts(mean)):
            parts_scr[pl.ds(group * 64 + s, 4, stride=8), :] = p[:4]
            parts_scr[pl.ds(group * 64 + 35 + s, 4, stride=8), :] = p[4:]
        for q in range(4):
            at = group * 64 + q * 8
            lhs = [parts_scr[at : at + 8, :], parts_scr[at + 32 : at + 40, :]]
            out = lax.dot_general(
                jnp.concatenate(lhs, axis=1).astype(bf16),
                inc_pair(group, q),
                (((1,), (1,)), ((), ())),
                preferred_element_type=f32,
            )
            for row, t in ((0, group * 8 + q), (3, group * 8 + q + 4)):
                part = out[row : row + 1] + out[row + 1 : row + 2] + out[row + 2 : row + 3]
                for k in range(K):
                    cover_ref[pl.ds(ids_ref[k, t], 1), :] += part[:, k * BLK : (k + 1) * BLK]
    soft_ref[...] = soft_sum


def first_kernel(
    ids_hbm, inc_hbm, cost_hbm, mult_hbm, upper,
    inc_ref, mean_ref, soft_ref, cover_ref, sum_ref, upper_ref,
    ids, raw, cost, mult, rows_scr, parts_scr, sems,
):
    tiles = cost.shape[0]
    small = [
        pltpu.make_async_copy(src, dst, sems.at[tiles + i])
        for i, (src, dst) in enumerate(((ids_hbm, ids), (mult_hbm, mult), (cost_hbm, cost)))
    ]
    large = [pltpu.make_async_copy(inc_hbm.at[t], raw.at[t], sems.at[t]) for t in range(tiles)]
    for copy in small:
        copy.start()
    for group in range(0, tiles, 8):
        for q in range(4):
            large[group + q].start()
            large[group + q + 4].start()
    for copy in small:
        copy.wait()
    seen = set()

    def inc_pair(group, q):
        pair = group * 4 + q
        if pair not in seen:
            seen.add(pair)
            for side in range(2):
                t = group * 8 + side * 4 + q
                large[t].wait()
                inc_ref[pair, :, side * TILE : (side + 1) * TILE] = (
                    raw[t].reshape(K * BLK, TILE).astype(f32).astype(inc_ref.dtype)
                )
        return inc_ref[pair]

    column_step(mult, ids, cost, inc_pair, None, rows_scr, parts_scr, mean_ref, soft_ref, cover_ref)
    sum_ref[...] = total_of(mult[...])
    upper_ref[...] = jnp.full(upper_ref.shape, upper[0], f32)


def total_of(v):
    n = v.shape[0] // 8
    v = v.reshape(n, 8, BLK)
    chains = [v[i] for i in range(4)]
    for i in range(4, n):
        chains[i % 4] = chains[i % 4] + v[i]
    return (chains[0] + chains[1]) + (chains[2] + chains[3])


def row_step(gathered, mult_ref, sum_ref, upper_ref, new_ref):
    norm, soft = [], sum_ref[...]
    lines = []
    for i in range(NEAR):
        slope = 1.0 - gathered[i * SLOT : i * SLOT + OWN, :]
        norm.append(slope * slope)
        lines.append(gathered[i * SLOT + OWN : (i + 1) * SLOT, :])
    value = jnp.sum(soft, keepdims=True) + jnp.sum(tree_sum(lines), keepdims=True)
    size = (upper_ref[:1, :1] - value) / (jnp.sum(tree_sum(norm), keepdims=True) + 1e-06)
    for i in range(NEAR):
        slope = 1.0 - gathered[i * SLOT : i * SLOT + OWN, :]
        here = slice(i * OWN, (i + 1) * OWN)
        new_ref[here, :] = jnp.maximum(0.0, mult_ref[here, :] + size * slope)


def next_kernel(
    gathered, mult_ref, sum_ref, upper_ref, ids_any, inc_ref, cost_ref, prev_ref,
    new_ref, mean_ref, soft_ref, cover_ref, total_ref, ids, rows_scr, parts_scr, sem,
):
    copy = pltpu.make_async_copy(ids_any, ids, sem)
    copy.start()
    row_step(gathered, mult_ref, sum_ref, upper_ref, new_ref)
    copy.wait()
    column_step(
        new_ref, ids, cost_ref, lambda group, q: inc_ref[group * 4 + q],
        prev_ref, rows_scr, parts_scr, mean_ref, soft_ref, cover_ref,
    )
    total_ref[...] = total_of(new_ref[...])


def last_kernel(gathered, mult_ref, sum_ref, upper_ref, mean_ref, new_ref, out_ref):
    out_ref[...] = mean_ref[...]
    row_step(gathered, mult_ref, sum_ref, upper_ref, new_ref)


def tree_sum(parts):
    while len(parts) > 1:
        parts = [a + b for a, b in zip(parts[::2], parts[1::2])]
    return parts[0]


def owner_kernel(in_ref, soft_ref, out_ref):
    total = tree_sum([in_ref[i] for i in range(NEAR)])
    soft = jnp.sum(soft_ref[...], axis=0, keepdims=True)
    for i in range(FAR):
        out_ref[i * SLOT : i * SLOT + OWN, :] = total
        out_ref[i * SLOT + OWN : (i + 1) * SLOT, :] = soft


def spread_kernel(in_ref, out_ref):
    total = tree_sum([in_ref[i * SLOT : i * SLOT + OWN, :] for i in range(FAR)])
    soft = tree_sum([in_ref[i * SLOT + OWN : (i + 1) * SLOT, :] for i in range(FAR)])
    for i in range(NEAR):
        out_ref[i * SLOT : i * SLOT + OWN, :] = total
        out_ref[i * SLOT + OWN : (i + 1) * SLOT, :] = soft


def call(kernel, name, out, specs, scratch=(), mib=8):
    return pl.pallas_call(
        kernel,
        out_shape=out,
        in_specs=specs,
        out_specs=jax.tree.map(lambda _: VMEM, out),
        scratch_shapes=scratch,
        compiler_params=pltpu.CompilerParams(vmem_limit_bytes=mib << 20),
        name=name,
    )


def exchange(blocks, groups):
    shape = blocks.shape
    blocks = blocks.reshape(len(groups[0]), -1)
    return lax.all_to_all(blocks, "d", 0, 0, tiled=True, axis_index_groups=groups).reshape(shape)


def local(block_ids, incidence, costs, start_mult, upper):
    tiles, rows = block_ids.shape[0], start_mult.shape[0]
    ids = block_ids.T

    def floats(*shape):
        return jax.ShapeDtypeStruct((*shape, BLK), f32)

    outs = (floats(tiles), floats(8), floats(rows), floats(8))
    scratch = [pltpu.VMEM((n, BLK), f32) for n in (tiles * K, tiles * 8 + 32)]
    inc, mean, soft, cover, total, top = call(
        first_kernel,
        "first",
        (jax.ShapeDtypeStruct((tiles // 2, K * BLK, 2 * TILE), INC), *outs, floats(8)),
        [HBM] * 4 + [pl.BlockSpec(memory_space=pltpu.SMEM)],
        [
            pltpu.SMEM((K, tiles), jnp.int32),
            pltpu.VMEM((tiles, K, BLK, TILE), jnp.int32),
            pltpu.VMEM((tiles, TILE), jnp.int32),
            pltpu.VMEM((rows, BLK), f32),
            *scratch,
            pltpu.SemaphoreType.DMA((tiles + 3,)),
        ],
        mib=16,
    )(*(pltpu.with_memory_space_constraint(a, pltpu.HBM) for a in (ids, incidence, costs, start_mult)), upper)
    mult = start_mult
    for step in range(ITERS):
        there = lax.all_to_all(
            cover.reshape(NEAR, OWN, BLK), "d", 0, 0, tiled=True, axis_index_groups=PLANES
        )
        there = call(owner_kernel, "owner", floats(FAR * SLOT), [VMEM] * 2)(there, soft)
        there = exchange(there, LINES)
        there = call(spread_kernel, "spread", floats(NEAR * SLOT), [VMEM])(there)
        rows_in = (exchange(there, PLANES), mult, total, top)
        if step < ITERS - 1:
            mult, mean, soft, cover, total = call(
                next_kernel,
                "next",
                (floats(rows), *outs),
                [VMEM] * 4 + [ANY] + [VMEM] * 3,
                [pltpu.SMEM((K, tiles), jnp.int32), *scratch, pltpu.SemaphoreType.DMA],
            )(*rows_in, ids, inc, costs, mean)
    return call(last_kernel, "last", (floats(rows), floats(tiles)), [VMEM] * 5)(*rows_in, mean)


def solution(mesh):
    return jax.shard_map(
        local,
        mesh=Mesh(mesh.devices.reshape(-1), ("d",)),
        in_specs=(
            P("d", None),
            P("d", None, None, None),
            P("d", None),
            P(),
            P(),
        ),
        out_specs=(P(), P("d", None)),
        check_vma=False,
    )
```
